128 devices in a mesh: data: 1, model: 2 (over core), seq: 64 (over z, y, x).
Axes of the slice: x: 4, y: 4, z: 4, core: 2. Of those that a mesh axis runs over, the one named last changes fastest.
Arguments:
- hidden: bfloat16 [64, 3584], P(('data', 'seq'))
- k_cache: bfloat16 [64, 8192, 4, 128], P('data', 'seq', 'model')
- v_cache: bfloat16 [64, 8192, 4, 128], P('data', 'seq', 'model')
- sel_blocks: int32 [64, 4, 32], P('data')
- g_attn: bfloat16 [3584], replicated
- g_mlp: bfloat16 [3584], replicated
- w_q: bfloat16 [3584, 3584], replicated
- w_o: bfloat16 [3584, 3584], replicated
- w_gate: bfloat16 [3584, 18944], P(None, 'model')
- w_up: bfloat16 [3584, 18944], P(None, 'model')
- w_down: bfloat16 [18944, 3584], P('model')
Outputs:
- output: bfloat16 [64, 3584], P(('data', 'seq'))
All inputs are finite; a program needn't handle non-finite values.
Results may differ from the reference program's by a relative error of at most 0.0123724.
Values are sent between devices in bfloat16 or wider.
A program may use at most 1 GiB of HBM per device.

```python
import jax
import jax.numpy as jnp
from jax import lax

MODEL_DIM = 3584
NUM_HEADS = 28
KV_HEADS = 4
HEAD_DIM = 128
FFN_DIM = 18944
BATCH_SIZE = 64
SEQ_LEN = 8192
TOP_BLOCKS = 32
HOLDERS = 64
BLOCK_CAP = 2
BLOCK_LEN = 64

NUM_BLOCKS = SEQ_LEN // BLOCK_LEN
BLOCKS_DEV = NUM_BLOCKS // HOLDERS
GROUP_SIZE = NUM_HEADS // KV_HEADS
NORM_EPS = 1e-5


def draw_selection(sel_key):
    sel_rows = BATCH_SIZE * KV_HEADS
    cand_count = HOLDERS * BLOCK_CAP
    key_pick, key_first, key_rest, key_order = jax.random.split(sel_key, 4)
    pick_score = jax.random.randint(key_pick, (sel_rows, HOLDERS, BLOCKS_DEV), 0, 65536)
    pick_score = pick_score * BLOCKS_DEV + jnp.arange(BLOCKS_DEV, dtype=jnp.int32)
    local_pick = jnp.argsort(pick_score, axis=-1)[:, :, :BLOCK_CAP]
    holder_ids = jnp.arange(HOLDERS, dtype=jnp.int32)
    candidates = (holder_ids[None, :, None] * BLOCKS_DEV + local_pick).reshape(sel_rows, cand_count)
    full_holder = jax.random.randint(key_first, (sel_rows, 1), 0, HOLDERS)
    cand_holder = jnp.repeat(holder_ids, BLOCK_CAP)[None, :]
    rest_score = jax.random.randint(key_rest, (sel_rows, cand_count), 1, 65536)
    rest_score = jnp.where(cand_holder == full_holder, 0, rest_score)
    rest_score = rest_score * cand_count + jnp.arange(cand_count, dtype=jnp.int32)
    chosen = jnp.take_along_axis(candidates, jnp.argsort(rest_score, axis=-1)[:, :TOP_BLOCKS], axis=-1)
    order_score = jax.random.randint(key_order, (sel_rows, TOP_BLOCKS), 0, 65536)
    order_score = order_score * TOP_BLOCKS + jnp.arange(TOP_BLOCKS, dtype=jnp.int32)
    chosen = jnp.take_along_axis(chosen, jnp.argsort(order_score, axis=-1), axis=-1)
    return chosen.reshape(BATCH_SIZE, KV_HEADS, TOP_BLOCKS).astype(jnp.int32)


def setup_inputs(seed: int = 0, part: int = 0) -> dict:
    base_key = jax.random.key(seed)
    part_key = jax.random.fold_in(base_key, part)
    key_x, key_kc, key_vc, key_sel = jax.random.split(part_key, 4)
    weight_keys = jax.random.split(jax.random.fold_in(base_key, 100003), 7)
    cache_shape = (BATCH_SIZE, SEQ_LEN, KV_HEADS, HEAD_DIM)
    wo_std = (TOP_BLOCKS * BLOCK_LEN / (6.0 * NUM_HEADS * HEAD_DIM)) ** 0.5
    hidden = jax.random.normal(key_x, (BATCH_SIZE, MODEL_DIM), jnp.float32)
    k_cache = jax.random.normal(key_kc, cache_shape, jnp.float32)
    v_cache = jax.random.normal(key_vc, cache_shape, jnp.float32)
    g_attn = 1.0 + 0.4 * jax.random.normal(weight_keys[0], (MODEL_DIM,), jnp.float32)
    g_mlp = 1.0 + 0.4 * jax.random.normal(weight_keys[1], (MODEL_DIM,), jnp.float32)
    w_q = jax.random.normal(weight_keys[2], (MODEL_DIM, NUM_HEADS * HEAD_DIM), jnp.float32) * MODEL_DIM ** -0.5
    w_o = jax.random.normal(weight_keys[3], (NUM_HEADS * HEAD_DIM, MODEL_DIM), jnp.float32) * wo_std
    w_gate = jax.random.normal(weight_keys[4], (MODEL_DIM, FFN_DIM), jnp.float32) * MODEL_DIM ** -0.5
    w_up = jax.random.normal(weight_keys[5], (MODEL_DIM, FFN_DIM), jnp.float32) * MODEL_DIM ** -0.5
    w_down = jax.random.normal(weight_keys[6], (FFN_DIM, MODEL_DIM), jnp.float32) * FFN_DIM ** -0.5
    return {
        "hidden": hidden.astype(jnp.bfloat16),
        "k_cache": k_cache.astype(jnp.bfloat16),
        "v_cache": v_cache.astype(jnp.bfloat16),
        "sel_blocks": draw_selection(key_sel),
        "g_attn": g_attn.astype(jnp.bfloat16),
        "g_mlp": g_mlp.astype(jnp.bfloat16),
        "w_q": w_q.astype(jnp.bfloat16),
        "w_o": w_o.astype(jnp.bfloat16),
        "w_gate": w_gate.astype(jnp.bfloat16),
        "w_up": w_up.astype(jnp.bfloat16),
        "w_down": w_down.astype(jnp.bfloat16),
    }


def rms_norm(hidden, gain_vec):
    hid_f32 = hidden.astype(jnp.float32)
    inv_rms = lax.rsqrt(jnp.mean(hid_f32 * hid_f32, axis=-1, keepdims=True) + NORM_EPS)
    return (hid_f32 * inv_rms * gain_vec.astype(jnp.float32)).astype(jnp.bfloat16)


def attend_one(operands):
    q_seq, k_seq, v_seq, sel_seq = operands
    k_blocks = k_seq.reshape(NUM_BLOCKS, BLOCK_LEN, KV_HEADS, HEAD_DIM)
    v_blocks = v_seq.reshape(NUM_BLOCKS, BLOCK_LEN, KV_HEADS, HEAD_DIM)
    pick_blocks = jax.vmap(lambda cache_h, idx_h: cache_h[idx_h], in_axes=(2, 0))
    k_sel = pick_blocks(k_blocks, sel_seq)
    v_sel = pick_blocks(v_blocks, sel_seq)
    scores = jnp.einsum("grd,gktd->grkt", q_seq.astype(jnp.float32), k_sel.astype(jnp.float32))
    top_score = jnp.max(scores, axis=(2, 3), keepdims=True)
    weights = jnp.exp(scores - top_score)
    exp_sum = jnp.sum(weights, axis=(2, 3))
    weighted = jnp.einsum("grkt,gktd->grd", weights.astype(jnp.bfloat16).astype(jnp.float32), v_sel.astype(jnp.float32))
    return (weighted / exp_sum[..., None]).astype(jnp.bfloat16)


def reference(hidden, k_cache, v_cache, sel_blocks, g_attn, g_mlp, w_q, w_o, w_gate, w_up, w_down):
    h_attn = rms_norm(hidden, g_attn)
    queries = (jnp.dot(h_attn, w_q, preferred_element_type=jnp.float32) * HEAD_DIM ** -0.5).astype(jnp.bfloat16)
    queries = queries.reshape(BATCH_SIZE, KV_HEADS, GROUP_SIZE, HEAD_DIM)
    attn_out = lax.map(attend_one, (queries, k_cache, v_cache, sel_blocks))
    attn_out = attn_out.reshape(BATCH_SIZE, NUM_HEADS * HEAD_DIM)
    resid_mid = (hidden.astype(jnp.float32) + jnp.dot(attn_out, w_o, preferred_element_type=jnp.float32)).astype(jnp.bfloat16)
    h_mlp = rms_norm(resid_mid, g_mlp)
    gate_act = jnp.dot(h_mlp, w_gate, preferred_element_type=jnp.float32).astype(jnp.bfloat16)
    up_act = jnp.dot(h_mlp, w_up, preferred_element_type=jnp.float32).astype(jnp.bfloat16)
    hidden_act = (jax.nn.silu(gate_act.astype(jnp.float32)) * up_act.astype(jnp.float32)).astype(jnp.bfloat16)
    return (resid_mid.astype(jnp.float32) + jnp.dot(hidden_act, w_down, preferred_element_type=jnp.float32)).astype(jnp.bfloat16)
```

```python
import functools

import jax
import jax.numpy as jnp
from jax import lax
from jax.experimental import pallas as pl
from jax.experimental.pallas import tpu as pltpu
from jax.sharding import PartitionSpec as P

MESH = pl.DeviceIdType.MESH
BLOCK_LEN = 64
NORM_EPS = 1e-5
LANES = 128
NEG_INF = float("-inf")
F32 = jnp.float32
BF16 = jnp.bfloat16


def row_iota(shape):
    return lax.broadcasted_iota(jnp.int32, shape, 0)


def decode_kernel(
    cfg,
    small_ref, sel_ref, k_hbm, v_hbm, wq_hbm, wo_hbm, wg_hbm, wu_hbm, wd_hbm,
    out_ref,
    k_buf, v_buf, wq_buf, wo_buf, wg_buf, wu_buf, wd_buf,
    hit_buf, lhs_buf, olhs_buf, q_all, part_out, part_in, stat_buf,
    pair_out, pair_in, h2_all, mlp_out, mlp_in, fin_out, fin_in,
    wq_sem, kv_sem, wo_sem, mlp_sem,
    q_send, q_recv, part_send, part_recv, pair_send, pair_recv, h2_send, h2_recv,
    red_send, red_recv, fin_send, fin_recv,
):
    seqs, plane, n_md, tiles_ffn, tiles_max = cfg
    planes = seqs // plane
    core = lax.axis_index("model")
    me = lax.axis_index("seq")
    my_plane = me // plane
    my_slot = me % plane
    heads = 14
    width = heads * LANES
    q_chunks = wq_buf.shape[0]
    o_chunks = wo_buf.shape[0]
    model_dim = n_md * LANES
    pad_md = small_ref.shape[1]

    def wq_copy(n):
        cols = pl.ds(pl.multiple_of(core * width + n * 256, LANES), 256)
        return pltpu.make_async_copy(wq_hbm.at[:, cols], wq_buf.at[n], wq_sem.at[n])

    def kv_copy(which, zz):
        src, dst = ((k_hbm, k_buf), (v_hbm, v_buf))[which]
        rows = pl.ds(zz * plane, plane)
        return pltpu.make_async_copy(src.at[rows], dst.at[rows], kv_sem.at[which, zz])

    def wo_copy(n):
        rows = pl.ds(pl.multiple_of(core * width, LANES), width)
        return pltpu.make_async_copy(wo_hbm.at[rows, pl.ds(n * 512, 512)], wo_buf.at[n], wo_sem.at[n])

    first_tile = (tiles_ffn * my_slot) // plane
    my_tiles = (tiles_ffn * (my_slot + 1)) // plane - first_tile
    ffn_cols = pl.ds(pl.multiple_of(first_tile * LANES, LANES), tiles_max * LANES)
    wg_copy = pltpu.make_async_copy(wg_hbm.at[:, ffn_cols], wg_buf, mlp_sem.at[0])
    wu_copy = pltpu.make_async_copy(wu_hbm.at[:, ffn_cols], wu_buf, mlp_sem.at[1])
    wd_copy = pltpu.make_async_copy(wd_hbm.at[ffn_cols, :], wd_buf, mlp_sem.at[2])

    for n in range(q_chunks):
        wq_copy(n).start()

    barrier = pltpu.get_barrier_semaphore()

    @pl.loop(1, seqs)
    def _(d):
        pl.semaphore_signal(barrier, inc=1, device_id={"seq": lax.rem(me + d, seqs)}, device_id_type=MESH)

    pl.semaphore_signal(barrier, inc=1, device_id={"model": 1 - core}, device_id_type=MESH)

    rows8 = row_iota((8, LANES))
    rows16 = row_iota((16, LANES))
    lane16 = lax.broadcasted_iota(jnp.int32, (16, LANES), 1)
    hid = small_ref[0].astype(F32)
    gain_attn = small_ref[1].astype(F32)
    gain_mlp = small_ref[2].astype(F32)

    def norm(x, gain):
        inv = lax.rsqrt(jnp.sum(x * x, keepdims=True) / model_dim + NORM_EPS)
        return (x * inv * gain).astype(BF16)

    h_attn = norm(hid, gain_attn).astype(F32)
    for n in range(n_md):
        lhs_buf[:, n * LANES:(n + 1) * LANES] = jnp.broadcast_to(h_attn[n:n + 1, :], (16, LANES)).astype(BF16)

    for j in range(2):
        block_id = me * 2 + j

        @pl.loop(0, seqs // 8)
        def _(b):
            sel = sel_ref[pl.ds(b * 8, 8)]
            found = jnp.max(jnp.where(sel == block_id, 1.0, 0.0), axis=2, keepdims=True)
            hit_buf[j, pl.ds(b * 8, 8)] = jnp.broadcast_to(jnp.where(found > 0.5, 0.0, NEG_INF), (8, 4, LANES))

    q_tile = jnp.zeros((16, LANES), F32)
    for n in range(q_chunks):
        wq_copy(n).wait()
        acc = jnp.dot(lhs_buf[...], wq_buf[n], preferred_element_type=F32) * (LANES ** -0.5)
        q_tile = jnp.where(rows16 == 2 * n, acc[:, :LANES], q_tile)
        q_tile = jnp.where(rows16 == 2 * n + 1, acc[:, LANES:], q_tile)
    q_all[me] = q_tile.astype(BF16)

    plane_order = [0, 1, planes - 1] + list(range(2, planes - 1)) if planes > 2 else list(range(planes))
    plane_ids = [lax.rem(my_plane + k, planes) for k in plane_order]
    for zz in plane_ids:
        kv_copy(0, zz).start()
        kv_copy(1, zz).start()
    for n in range(o_chunks):
        wo_copy(n).start()
    wg_copy.start()
    wu_copy.start()
    wd_copy.start()

    pl.semaphore_wait(barrier, seqs)

    def q_push(to):
        return pltpu.make_async_remote_copy(
            src_ref=q_all.at[me], dst_ref=q_all.at[me], send_sem=q_send, recv_sem=q_recv.at[my_plane],
            device_id={"seq": to}, device_id_type=MESH)

    @pl.loop(1, plane)
    def _(d):
        q_push(my_plane * plane + lax.rem(my_slot + d, plane)).start()

    for zz in plane_ids[1:]:
        @pl.loop(0, plane)
        def _(d):
            q_push(zz * plane + lax.rem(my_slot + d, plane)).start()

    parity = ((lane16 % 2) == jnp.where(rows16 < 7, 0, 1)) & (rows16 < heads)

    def part_push(to):
        return pltpu.make_async_remote_copy(
            src_ref=part_out.at[to], dst_ref=part_in.at[me], send_sem=part_send, recv_sem=part_recv,
            device_id={"seq": to}, device_id_type=MESH)

    for k, zz in enumerate(plane_ids):
        base = zz * plane
        if k == 0:
            if plane > 1:
                gone = q_all.at[pl.ds(0, plane - 1)]
                pltpu.make_async_copy(gone, gone, q_recv.at[zz]).wait()
        else:
            whole = q_all.at[pl.ds(0, plane)]
            pltpu.make_async_copy(whole, whole, q_recv.at[zz]).wait()
        kv_copy(0, zz).wait()
        kv_copy(1, zz).wait()
        stats = jnp.zeros((16, LANES), F32)
        for i in range(plane):
            row = base + i
            scores = lax.dot_general(q_all[row], k_buf[row], (((1,), (1,)), ((), ())), preferred_element_type=F32)
            masked = []
            for j in range(2):
                hit_0 = jnp.broadcast_to(hit_buf[j, row, pl.ds(2 * core, 1), :], (16, LANES))
                hit_1 = jnp.broadcast_to(hit_buf[j, row, pl.ds(2 * core + 1, 1), :], (16, LANES))
                bias = jnp.where(parity, jnp.where(rows16 < 7, hit_0, hit_1), NEG_INF)
                masked.append(scores[:, j * LANES:(j + 1) * LANES] + bias)
            top = jnp.max(jnp.maximum(masked[0], masked[1]), axis=1, keepdims=True)
            safe = jnp.where(top == NEG_INF, 0.0, top)
            exps = [jnp.exp(s - safe) for s in masked]
            total = jnp.sum(exps[0] + exps[1], axis=1, keepdims=True)
            weights = jnp.concatenate([e.astype(BF16) for e in exps], axis=1)
            part_out[row] = jnp.dot(weights, v_buf[row], preferred_element_type=F32)
            stats = jnp.where(lane16 == i, top, stats)
            stats = jnp.where(lane16 == plane + i, total, stats)
        stats_t = stats.T
        for i in range(plane):
            row = base + i
            part_out[row, 14:15, 0:16] = stats_t[i:i + 1, :]
            part_out[row, 15:16, 0:16] = stats_t[plane + i:plane + i + 1, :]
        for i in range(plane):
            if k == 0:
                @pl.when(i != my_slot)
                def _():
                    part_push(base + i).start()
            else:
                part_push(base + i).start()

    part_in[me] = part_out[me]
    others = part_in.at[pl.ds(0, seqs - 1)]
    pltpu.make_async_copy(others, others, part_recv).wait()
    for i in range(seqs):
        stat_buf[i:i + 1, :] = part_in[i, 14:15, :]
    head_lane = lax.broadcasted_iota(jnp.int32, (seqs, LANES), 1) < heads
    tops = jnp.where(head_lane, stat_buf[0:seqs, :], 0.0)
    scale = jnp.exp(tops - jnp.max(tops, axis=0, keepdims=True))
    for i in range(seqs):
        stat_buf[i:i + 1, :] = part_in[i, 15:16, :]
    sums = jnp.where(head_lane, stat_buf[0:seqs, :], 0.0)
    denom = jnp.sum(scale * sums, axis=0, keepdims=True)
    stat_buf[0:seqs, :] = scale
    stat_buf[seqs:seqs + 8, :] = jnp.broadcast_to(denom, (8, LANES))
    scale_t = stat_buf[...].T
    acc = jnp.zeros((16, LANES), F32)
    for i in range(seqs):
        acc = acc + scale_t[0:16, i:i + 1] * part_in[i]
    attn = (acc / jnp.where(rows16 < heads, scale_t[0:16, seqs:seqs + 1], 1.0)).astype(BF16).astype(F32)
    for r in range(heads):
        olhs_buf[:, r * LANES:(r + 1) * LANES] = jnp.broadcast_to(attn[r:r + 1, :], (16, LANES)).astype(BF16)

    proj = [jnp.zeros((8, LANES), F32) for _ in range(pad_md // 8)]
    for n in range(o_chunks):
        wo_copy(n).wait()
        acc = jnp.dot(olhs_buf[...], wo_buf[n], preferred_element_type=F32)
        for t in range(4):
            r = 4 * n + t
            proj[r // 8] = jnp.where(rows8 == r % 8, acc[0:8, t * LANES:(t + 1) * LANES], proj[r // 8])
    for r in range(pad_md // 8):
        pair_out[r * 8:(r + 1) * 8, :] = proj[r]
    pair = pltpu.make_async_remote_copy(
        src_ref=pair_out, dst_ref=pair_in, send_sem=pair_send, recv_sem=pair_recv,
        device_id={"model": 1 - core}, device_id_type=MESH)
    pair.start()
    pair.wait()
    resid = (hid + (pair_out[...] + pair_in[...])).astype(BF16).astype(F32)
    h2_all[my_slot] = norm(resid, gain_mlp)

    def h2_push(to_slot):
        return pltpu.make_async_remote_copy(
            src_ref=h2_all.at[my_slot], dst_ref=h2_all.at[my_slot], send_sem=h2_send, recv_sem=h2_recv,
            device_id={"seq": my_plane * plane + to_slot}, device_id_type=MESH)

    @pl.loop(1, plane)
    def _(d):
        h2_push(lax.rem(my_slot + d, plane)).start()

    gone = h2_all.at[pl.ds(0, plane - 1)]
    pltpu.make_async_copy(gone, gone, h2_recv).wait()
    rows = [h2_all[i].astype(F32) for i in range(plane)]
    for n in range(n_md):
        tile = jnp.zeros((16, LANES), F32)
        for i in range(plane):
            tile = jnp.where(rows16 == i, jnp.broadcast_to(rows[i][n:n + 1, :], (16, LANES)), tile)
        lhs_buf[:, n * LANES:(n + 1) * LANES] = tile.astype(BF16)

    wg_copy.wait()
    gate = jnp.dot(lhs_buf[...], wg_buf[...], preferred_element_type=F32).astype(BF16).astype(F32)
    wu_copy.wait()
    up = jnp.dot(lhs_buf[...], wu_buf[...], preferred_element_type=F32).astype(BF16).astype(F32)
    act = jax.nn.silu(gate) * up
    cols = lax.broadcasted_iota(jnp.int32, act.shape, 1)
    act = jnp.where(cols < my_tiles * LANES, act, 0.0).astype(BF16)
    wd_copy.wait()
    for n in range(o_chunks):
        acc = jnp.dot(act, wd_buf[:, n * 512:(n + 1) * 512], preferred_element_type=F32)
        for t in range(4):
            for i in range(plane):
                mlp_out[i, 4 * n + t:4 * n + t + 1, :] = acc[i:i + 1, t * LANES:(t + 1) * LANES]

    def red_push(to_slot):
        return pltpu.make_async_remote_copy(
            src_ref=mlp_out.at[to_slot], dst_ref=mlp_in.at[my_slot], send_sem=red_send, recv_sem=red_recv,
            device_id={"seq": my_plane * plane + to_slot}, device_id_type=MESH)

    @pl.loop(1, plane)
    def _(d):
        red_push(lax.rem(my_slot + d, plane)).start()

    mlp_in[my_slot] = mlp_out[my_slot]
    others = mlp_in.at[pl.ds(0, plane - 1)]
    pltpu.make_async_copy(others, others, red_recv).wait()
    total = mlp_in[0]
    for i in range(1, plane):
        total = total + mlp_in[i]
    fin_out[...] = total
    fin = pltpu.make_async_remote_copy(
        src_ref=fin_out, dst_ref=fin_in, send_sem=fin_send, recv_sem=fin_recv,
        device_id={"model": 1 - core}, device_id_type=MESH)
    fin.start()
    fin.wait()
    out_ref[0:n_md, :] = (resid[0:n_md, :] + (fin_out[...] + fin_in[...])).astype(BF16)

    pltpu.make_async_copy(q_all.at[pl.ds(0, seqs - 1)], q_all.at[pl.ds(0, seqs - 1)], q_send).wait()
    pltpu.make_async_copy(others_part(part_in, seqs), others_part(part_in, seqs), part_send).wait()
    pltpu.make_async_copy(gone, gone, h2_send).wait()
    pltpu.make_async_copy(others, others, red_send).wait()


def others_part(ref, seqs):
    return ref.at[pl.ds(0, seqs - 1)]


def plane_size(seq_devs):
    return 16 if seq_devs % 16 == 0 else 4


def solution(mesh):
    model_devs = mesh.shape["model"]
    seq_devs = mesh.shape["seq"]

    def device_step(hidden, k_cache, v_cache, sel_blocks, g_attn, g_mlp, w_q, w_o, w_gate, w_up, w_down):
        model_dim = hidden.shape[1]
        batch, tokens, kv_local, head_dim = k_cache.shape
        n_md = model_dim // LANES
        pad_md = -(-n_md // 16) * 16
        plane = plane_size(seq_devs)
        tiles_ffn = w_gate.shape[1] // LANES
        tiles_max = -(-tiles_ffn // plane)
        width = w_q.shape[1] // model_devs
        small = jnp.stack([hidden.reshape(n_md, LANES), g_attn.reshape(n_md, LANES), g_mlp.reshape(n_md, LANES)])
        small = jnp.pad(small, ((0, 0), (0, pad_md - n_md), (0, 0)))
        kv_rows = tokens * kv_local
        k_rows = k_cache.reshape(batch, kv_rows, head_dim)
        v_rows = v_cache.reshape(batch, kv_rows, head_dim)
        cfg = (seq_devs, plane, n_md, tiles_ffn, tiles_max)
        any_spec = pl.BlockSpec(memory_space=pl.ANY)
        vmem_spec = pl.BlockSpec(memory_space=pltpu.VMEM)
        dma = pltpu.SemaphoreType.DMA
        out = pl.pallas_call(
            functools.partial(decode_kernel, cfg),
            out_shape=jax.ShapeDtypeStruct((n_md, LANES), BF16),
            in_specs=[vmem_spec, vmem_spec] + [any_spec] * 7,
            out_specs=vmem_spec,
            scratch_shapes=[
                pltpu.VMEM((batch, kv_rows, LANES), BF16),
                pltpu.VMEM((batch, kv_rows, LANES), BF16),
                pltpu.VMEM((width // 256, model_dim, 256), BF16),
                pltpu.VMEM((model_dim // 512, width, 512), BF16),
                pltpu.VMEM((model_dim, tiles_max * LANES), BF16),
                pltpu.VMEM((model_dim, tiles_max * LANES), BF16),
                pltpu.VMEM((tiles_max * LANES, model_dim), BF16),
                pltpu.VMEM((2, batch, 4, LANES), F32),
                pltpu.VMEM((16, model_dim), BF16),
                pltpu.VMEM((16, width), BF16),
                pltpu.VMEM((batch, 16, LANES), BF16),
                pltpu.VMEM((batch, 16, LANES), F32),
                pltpu.VMEM((batch, 16, LANES), F32),
                pltpu.VMEM((seq_devs + 8, LANES), F32),
                pltpu.VMEM((pad_md, LANES), F32),
                pltpu.VMEM((pad_md, LANES), F32),
                pltpu.VMEM((plane, pad_md, LANES), BF16),
                pltpu.VMEM((plane, n_md, LANES), F32),
                pltpu.VMEM((plane, n_md, LANES), F32),
                pltpu.VMEM((n_md, LANES), F32),
                pltpu.VMEM((n_md, LANES), F32),
                dma((width // 256,)), dma((2, seq_devs // plane)), dma((model_dim // 512,)), dma((3,)),
                dma, dma((seq_devs // plane,)), dma, dma, dma, dma, dma, dma, dma, dma, dma, dma,
            ],
            compiler_params=pltpu.CompilerParams(
                collective_id=0, has_side_effects=True, vmem_limit_bytes=64 * 1024 * 1024 - 128 * 1024),
            name="decode_step",
        )(small, sel_blocks, k_rows, v_rows, w_q, w_o, w_gate, w_up, w_down)
        return out.reshape(1, model_dim)

    cache_spec = P("data", "seq", "model", None)
    in_specs = (P(("data", "seq"), None), cache_spec, cache_spec, P("data", None, None), P(None), P(None), P(None, None), P(None, None), P(None, "model"), P(None, "model"), P("model", None))
    return jax.shard_map(device_step, mesh=mesh, in_specs=in_specs, out_specs=P(("data", "seq"), None), check_vma=False)
```

```python
import functools

import jax
import jax.numpy as jnp
from jax import lax
from jax.experimental import pallas as pl
from jax.experimental.pallas import tpu as pltpu
from jax.sharding import PartitionSpec as P

MESH = pl.DeviceIdType.MESH
BLOCK_LEN = 64
NORM_EPS = 1e-5
LANES = 128
NEG_INF = float("-inf")
F32 = jnp.float32
BF16 = jnp.bfloat16


def row_iota(shape):
    return lax.broadcasted_iota(jnp.int32, shape, 0)


def torus_dims(seq_devs):
    side = round(seq_devs ** (1 / 3))
    return (side, side, side)


def mlp_box(dims):
    return (dims[0], 2, 2) if dims[0] > 2 else (2, 2, 1)


def offset_groups(dims):
    offsets = [(a, b, c) for a in range(dims[0]) for b in range(dims[1]) for c in range(dims[2])]

    def hops(o):
        return sum(min(d, n - d) for d, n in zip(o, dims))

    top = sum(n // 2 for n in dims)
    if top >= 6:
        bands = [(0, 1, 2), (3,), (6, 5), (4,)]
        push_bands = [(0, 1, 2), (6, 5), (4,), (3,)]
    else:
        bands = push_bands = [(0, 1), (2,), (3,)]
    pick = [[o for h in band for o in offsets if hops(o) == h] for band in bands]
    push = [o for band in push_bands for h in band for o in offsets if hops(o) == h]
    return push, pick


def decode_kernel(
    cfg,
    hid_hbm, ga_hbm, gm_hbm, sel_hbm, k_hbm, v_hbm, wq_hbm, wo_hbm, wg_hbm, wu_hbm, wd_hbm,
    out_ref,
    k_buf, v_buf, wq_buf, wo_buf, wg_buf, wu_buf, wd_buf,
    hid_ref, ga_ref, gm_ref, sel_ref, hit_buf, lhs_buf, olhs_buf,
    q_out, q_all, s_buf, p_buf, part_out, part_in, stat_buf,
    pair_out, pair_in, h2_all, mlp_out, mlp_in, fin_out, fin_in,
    small_sem, wq_sem, kv_sem, wo_sem, mlp_sem,
    q_send, q_recv, part_send, part_recv, pair_send, pair_recv, h2_send, h2_recv,
    red_send, red_recv, fin_send, fin_recv,
):
    seqs, n_md, tiles_ffn, tiles_max = cfg
    dims = torus_dims(seqs)
    box = mlp_box(dims)
    members = box[0] * box[1] * box[2]
    push_order, groups = offset_groups(dims)
    core = lax.axis_index("model")
    other = 1 - core
    me = lax.axis_index("seq")
    place = (me // (dims[1] * dims[2]), (me // dims[2]) % dims[1], me % dims[2])

    def seq_at(offset):
        z, y, x = (lax.rem(p + o, n) if o else p for p, o, n in zip(place, offset, dims))
        return (z * dims[1] + y) * dims[2] + x

    inner = tuple(p % n for p, n in zip(place, box))
    my_slot = (inner[0] * box[1] + inner[1]) * box[2] + inner[2]

    def member_at(offset):
        z, y, x = (lax.rem(p + o, n) if o else p for p, o, n in zip(inner, offset, box))
        slot = (z * box[1] + y) * box[2] + x
        whole = [p - i + v for p, i, v in zip(place, inner, (z, y, x))]
        return slot, (whole[0] * dims[1] + whole[1]) * dims[2] + whole[2]

    def box_hops(o):
        return sum(min(d, n - d) for d, n in zip(o, box))

    box_offsets = [(a, b, c) for a in range(box[0]) for b in range(box[1]) for c in range(box[2])]
    box_far_first = sorted(box_offsets, key=lambda o: (-box_hops(o), o))

    heads = 14
    width = heads * LANES
    q_chunks = -(-wq_buf.shape[1] // 512)
    o_chunks = wo_buf.shape[0]
    model_dim = n_md * LANES
    pad_md = pair_out.shape[0]
    k_parts = 4
    part_rows = model_dim // k_parts

    wq_cols = [(c, min(512, width - c)) for c in range(0, width, 512)]

    def wq_start(n):
        at, size = wq_cols[n]
        cols = pl.ds(pl.multiple_of(other * width + at, LANES), size)
        for part in range(k_parts):
            rows = pl.ds(part * part_rows, part_rows)
            pltpu.make_async_copy(wq_hbm.at[rows, cols], wq_buf.at[rows, pl.ds(at, size)], wq_sem.at[n]).start()

    def wq_wait(n):
        at, size = wq_cols[n]
        done = wq_buf.at[:, pl.ds(at, size)]
        pltpu.make_async_copy(done, done, wq_sem.at[n]).wait()

    kv_parts = 4
    kv_rows = seqs // kv_parts

    def kv_start(which):
        src, dst = ((k_hbm, k_buf), (v_hbm, v_buf))[which]
        for part in range(kv_parts):
            rows = pl.ds(part * kv_rows, kv_rows)
            pltpu.make_async_copy(src.at[rows], dst.at[rows], kv_sem.at[which]).start()

    def kv_wait(which):
        dst = (k_buf, v_buf)[which]
        pltpu.make_async_copy(dst, dst, kv_sem.at[which]).wait()

    def wo_copy(n):
        rows = pl.ds(pl.multiple_of(other * width, LANES), width)
        return pltpu.make_async_copy(wo_hbm.at[rows, pl.ds(n * 512, 512)], wo_buf.at[n], wo_sem.at[n])

    first_tile = (tiles_ffn * my_slot) // members
    my_tiles = (tiles_ffn * (my_slot + 1)) // members - first_tile
    ffn_cols = pl.ds(pl.multiple_of(first_tile * LANES, LANES), tiles_max * LANES)

    def up_start(which):
        src, dst = ((wg_hbm, wg_buf), (wu_hbm, wu_buf))[which]
        for part in range(k_parts):
            rows = pl.ds(part * part_rows, part_rows)
            pltpu.make_async_copy(src.at[rows, ffn_cols], dst.at[rows], mlp_sem.at[which]).start()

    def up_wait(which):
        dst = (wg_buf, wu_buf)[which]
        pltpu.make_async_copy(dst, dst, mlp_sem.at[which]).wait()

    wd_copy = pltpu.make_async_copy(wd_hbm.at[ffn_cols, :], wd_buf, mlp_sem.at[2])

    smalls = [
        pltpu.make_async_copy(src, dst, small_sem.at[n])
        for n, (src, dst) in enumerate(((hid_hbm, hid_ref), (ga_hbm, ga_ref), (gm_hbm, gm_ref), (sel_hbm, sel_ref)))
    ]
    for copy in smalls[:2]:
        copy.start()

    barrier = pltpu.get_barrier_semaphore()

    def greet(d):
        pl.semaphore_signal(barrier, inc=1, device_id={"model": other, "seq": lax.rem(me + d, seqs)}, device_id_type=MESH)

    early = seqs // 4
    pl.loop(0, early)(greet)
    for n in range(q_chunks):
        wq_start(n)
    for copy in smalls[2:]:
        copy.start()
    pl.loop(early, seqs)(greet)

    smalls[0].wait()
    smalls[1].wait()
    rows8 = row_iota((8, LANES))
    rows16 = row_iota((16, LANES))
    lane16 = lax.broadcasted_iota(jnp.int32, (16, LANES), 1)
    hid_parts = [jnp.zeros((8, LANES), F32) for _ in range(pad_md // 8)]
    for n in range(n_md):
        piece = jnp.broadcast_to(hid_ref[:, n * LANES:(n + 1) * LANES].astype(F32), (8, LANES))
        hid_parts[n // 8] = jnp.where(rows8 == n % 8, piece, hid_parts[n // 8])
    hid = jnp.concatenate(hid_parts, axis=0)
    fill = jnp.zeros((pad_md - n_md, LANES), F32)

    def norm(x, gain_ref):
        inv = lax.rsqrt(jnp.sum(x * x, keepdims=True) / model_dim + NORM_EPS)
        return (x * inv * jnp.concatenate([gain_ref[...].astype(F32), fill], axis=0)).astype(BF16)

    h_attn = norm(hid, ga_ref).astype(F32)
    for n in range(n_md):
        lhs_buf[:, n * LANES:(n + 1) * LANES] = jnp.broadcast_to(h_attn[n:n + 1, :], (16, LANES)).astype(BF16)

    q_tile = jnp.zeros((16, LANES), F32)
    head = 0
    for n in range(q_chunks):
        wq_wait(n)
        if n == q_chunks - 3:
            kv_start(0)
        if n == q_chunks - 2:
            kv_start(1)
        at, size = wq_cols[n]
        acc = jnp.dot(lhs_buf[...], wq_buf[:, at:at + size], preferred_element_type=F32) * (LANES ** -0.5)
        for t in range(size // LANES):
            q_tile = jnp.where(rows16 == head + head // 7, acc[:, t * LANES:(t + 1) * LANES], q_tile)
            head += 1
    q_out[...] = q_tile.astype(BF16)

    pl.semaphore_wait(barrier, seqs)

    def group_of(offset):
        back = tuple((n - o) % n for o, n in zip(offset, dims))
        return [k for k, group in enumerate(groups) if back in group][0]

    for offset in push_order:
        pltpu.make_async_remote_copy(
            src_ref=q_out, dst_ref=q_all.at[me], send_sem=q_send, recv_sem=q_recv.at[group_of(offset)],
            device_id={"model": other, "seq": seq_at(offset)}, device_id_type=MESH).start()
    for n in range(o_chunks):
        wo_copy(n).start()
    up_start(0)
    up_start(1)
    wd_copy.start()

    stat_buf[...] = jnp.zeros((LANES, LANES), F32)
    smalls[3].wait()
    for j in range(2):
        found = [
            jnp.max(jnp.where(sel_ref[g] == me * 2 + j, 1.0, 0.0), axis=0, keepdims=True)
            for g in range(4)
        ]
        for g in range(2):
            mine = jnp.where(core == 0, found[g], found[2 + g])
            column = jnp.broadcast_to(mine, (8, seqs)).T[:, 0:1]
            hit_buf[j, g] = jnp.broadcast_to(jnp.where(column > 0.5, 0.0, NEG_INF), (seqs, LANES))

    parity = ((lane16 % 2) == jnp.where(rows16 < 8, 0, 1)) & (rows16 % 8 != 7)
    order = [(k, i, seq_at(offset)) for k, group in enumerate(groups) for i, offset in enumerate(group)]
    tops = {}
    stats = {k: [jnp.zeros((16, LANES), F32)] * 2 for k in range(len(groups))}
    gap = 5
    slots = [None]
    for n, item in enumerate(order):
        if item[1] == 0 and item[0] == 1:
            slots += [None] * (3 * gap)
        slots.append((n,) + item)
    slots += [None] * (3 * gap)

    def spot(n):
        return slice(n * 16, (n + 1) * 16)

    def push_half(row, half):
        tile = pl.ds(half * 8, 8)
        pltpu.make_async_remote_copy(
            src_ref=part_out.at[row, tile], dst_ref=part_in.at[me, tile], send_sem=part_send, recv_sem=part_recv.at[half],
            device_id={"model": other, "seq": row}, device_id_type=MESH).start()

    def score_stage(n, k, i, row):
        if i == 0:
            arrived = q_all.at[pl.ds(0, len(groups[k]))]
            pltpu.make_async_copy(arrived, arrived, q_recv.at[k]).wait()
        if n == 0:
            kv_wait(0)
        scores = lax.dot_general(q_all[row], k_buf[row], (((1,), (1,)), ((), ())), preferred_element_type=F32)
        for j in range(2):
            hit_0 = jnp.broadcast_to(hit_buf[j, 0, pl.ds(row, 1), :], (16, LANES))
            hit_1 = jnp.broadcast_to(hit_buf[j, 1, pl.ds(row, 1), :], (16, LANES))
            bias = jnp.where(parity, jnp.where(rows16 < 8, hit_0, hit_1), NEG_INF)
            s_buf[spot(n), j * LANES:(j + 1) * LANES] = scores[:, j * LANES:(j + 1) * LANES] + bias

    def top_stage(n, k, i, row):
        tops[n] = jnp.max(s_buf[spot(n), :], axis=1, keepdims=True)

    def exp_stage(n, k, i, row):
        top = tops.pop(n)
        safe = jnp.where(top == NEG_INF, 0.0, top)
        exps = jnp.exp(s_buf[spot(n), :] - safe)
        p_buf[spot(n), :] = exps.astype(BF16)
        total = jnp.sum(exps, axis=1, keepdims=True)
        stats[k] = [jnp.where(lane16 == i, v, old) for v, old in zip((top, total), stats[k])]

    def value_stage(n, k, i, row):
        if n == 0:
            kv_wait(1)
        part_out[row] = jnp.dot(p_buf[spot(n), :], v_buf[row], preferred_element_type=F32)
        if i == len(groups[k]) - 1:
            stats_t = jnp.concatenate(stats[k], axis=0).T
            rows = [item[2] for item in order if item[0] == k]
            for m, to in enumerate(rows):
                part_out[to, 7:8, 0:32] = stats_t[m:m + 1, :]
                part_out[to, 15:16, 0:32] = stats_t[m:m + 1, :]
            for to in rows:
                push_half(to, 0)
            if k == 0:
                for to in rows:
                    push_half(to, 1)

    for t in range(len(slots)):
        for lag, stage in ((0, score_stage), (gap, top_stage), (2 * gap, exp_stage), (3 * gap, value_stage)):
            if t >= lag and slots[t - lag] is not None:
                stage(*slots[t - lag])
    for k in range(len(groups) - 1, 0, -1):
        for item in order:
            if item[0] == k:
                push_half(item[2], 1)

    proj = [jnp.zeros((8, LANES), F32) for _ in range(pad_md // 8)]
    half_width = width // 2
    for half in range(2):
        tile = slice(half * 8, half * 8 + 8)
        landed = part_in.at[:, pl.ds(half * 8, 8)]
        pltpu.make_async_copy(landed, landed, part_recv.at[half]).wait()
        for i in range(seqs):
            stat_buf[i:i + 1, :] = part_in[i, half * 8 + 7:half * 8 + 8, :]
        stat_t = stat_buf[...].T
        real = lax.broadcasted_iota(jnp.int32, (8, LANES), 1) < seqs
        top = jnp.where(real, stat_t[tile, :], NEG_INF)
        scale = jnp.exp(top - jnp.max(top, axis=1, keepdims=True))
        mass = jnp.where(real, stat_t[half * 8 + 16:half * 8 + 24, :], 0.0)
        denom = jnp.sum(scale * mass, axis=1, keepdims=True)
        sums = [jnp.zeros((8, LANES), F32) for _ in range(4)]
        for i in range(seqs):
            sums[i % 4] = sums[i % 4] + scale[:, i:i + 1] * part_in[i, tile, :]
        attn = (((sums[0] + sums[1]) + (sums[2] + sums[3])) / denom).astype(BF16).astype(F32)
        for r in range(7):
            olhs_buf[:, r * LANES:(r + 1) * LANES] = jnp.broadcast_to(attn[r:r + 1, :], (16, LANES)).astype(BF16)
        for n in range(o_chunks):
            if half == 0:
                wo_copy(n).wait()
            acc = jnp.dot(olhs_buf[...], wo_buf[n, half * half_width:(half + 1) * half_width, :], preferred_element_type=F32)
            for t in range(4):
                r = 4 * n + t
                here = jnp.where(rows8 == r % 8, acc[0:8, t * LANES:(t + 1) * LANES], 0.0)
                proj[r // 8] = proj[r // 8] + here
    for r in range(pad_md // 8):
        pair_out[r * 8:(r + 1) * 8, :] = proj[r]
    pair = pltpu.make_async_remote_copy(
        src_ref=pair_out, dst_ref=pair_in, send_sem=pair_send, recv_sem=pair_recv,
        device_id={"model": other}, device_id_type=MESH)
    pair.start()
    pair.wait()
    smalls[2].wait()
    resid = (hid + (pair_out[...] + pair_in[...])).astype(BF16).astype(F32)
    h2_all[my_slot] = norm(resid, gm_ref)

    for offset in box_far_first:
        if any(offset):
            pltpu.make_async_remote_copy(
                src_ref=h2_all.at[my_slot], dst_ref=h2_all.at[my_slot], send_sem=h2_send, recv_sem=h2_recv,
                device_id={"model": other, "seq": member_at(offset)[1]}, device_id_type=MESH).start()
    gone = h2_all.at[pl.ds(0, members - 1)]
    pltpu.make_async_copy(gone, gone, h2_recv).wait()
    rows = [h2_all[i].astype(F32) for i in range(members)]
    for n in range(n_md):
        tile = jnp.zeros((16, LANES), F32)
        for i in range(members):
            tile = jnp.where(rows16 == i, jnp.broadcast_to(rows[i][n:n + 1, :], (16, LANES)), tile)
        lhs_buf[:, n * LANES:(n + 1) * LANES] = tile.astype(BF16)

    up_wait(0)
    gate = jnp.dot(lhs_buf[...], wg_buf[...], preferred_element_type=F32).astype(BF16).astype(F32)
    up_wait(1)
    up = jnp.dot(lhs_buf[...], wu_buf[...], preferred_element_type=F32).astype(BF16).astype(F32)
    act = jax.nn.silu(gate) * up
    cols = lax.broadcasted_iota(jnp.int32, act.shape, 1)
    act = jnp.where(cols < my_tiles * LANES, act, 0.0).astype(BF16)
    wd_copy.wait()
    cut = min(16, n_md // 2 // 4 * 4) if n_md > 4 else 0
    pieces = [(0, cut), (cut, n_md)] if cut else [(0, n_md)]
    homes = [member_at(offset) for offset in box_far_first]
    for piece, (low, high) in enumerate(pieces):
        for n in range(low // 4, high // 4):
            acc = jnp.dot(act, wd_buf[:, n * 512:(n + 1) * 512], preferred_element_type=F32)
            for t in range(4):
                for i in range(members):
                    mlp_out[i, 4 * n + t:4 * n + t + 1, :] = acc[i:i + 1, t * LANES:(t + 1) * LANES]
        for slot, home in homes:
            tile = pl.ds(low, high - low)
            pltpu.make_async_remote_copy(
                src_ref=mlp_out.at[slot, tile], dst_ref=mlp_in.at[my_slot, tile], send_sem=red_send, recv_sem=red_recv.at[piece],
                device_id={"model": other, "seq": home}, device_id_type=MESH).start()

    finals = []
    for piece, (low, high) in enumerate(pieces):
        tile = pl.ds(low, high - low)
        landed = mlp_in.at[:, tile]
        pltpu.make_async_copy(landed, landed, red_recv.at[piece]).wait()
        total = mlp_in[0, low:high, :]
        for i in range(1, members):
            total = total + mlp_in[i, low:high, :]
        fin_out[low:high, :] = total
        fin = pltpu.make_async_remote_copy(
            src_ref=fin_out.at[tile], dst_ref=fin_in.at[tile], send_sem=fin_send.at[piece], recv_sem=fin_recv.at[piece],
            device_id={"model": other}, device_id_type=MESH)
        fin.start()
        finals.append(fin)
    for fin in finals:
        fin.wait()
    result = resid[0:n_md, :] + (fin_out[...] + fin_in[...])
    for n in range(n_md):
        out_ref[:, n * LANES:(n + 1) * LANES] = result[n:n + 1, :].astype(BF16)

    pltpu.make_async_copy(q_all, q_all, q_send).wait()
    pltpu.make_async_copy(part_in, part_in, part_send).wait()
    pltpu.make_async_copy(gone, gone, h2_send).wait()
    pltpu.make_async_copy(mlp_in, mlp_in, red_send).wait()


def solution(mesh):
    model_devs = mesh.shape["model"]
    seq_devs = mesh.shape["seq"]

    def device_step(hidden, k_cache, v_cache, sel_blocks, g_attn, g_mlp, w_q, w_o, w_gate, w_up, w_down):
        model_dim = hidden.shape[1]
        batch, tokens, kv_local, head_dim = k_cache.shape
        n_md = model_dim // LANES
        pad_md = -(-n_md // 16) * 16
        dims = torus_dims(seq_devs)
        box = mlp_box(dims)
        members = box[0] * box[1] * box[2]
        tiles_ffn = w_gate.shape[1] // LANES
        tiles_max = -(-tiles_ffn // members)
        width = w_q.shape[1] // model_devs
        kv_rows = tokens * kv_local
        k_rows = k_cache.reshape(batch, kv_rows, head_dim)
        v_rows = v_cache.reshape(batch, kv_rows, head_dim)
        cfg = (seq_devs, n_md, tiles_ffn, tiles_max)
        any_spec = pl.BlockSpec(memory_space=pl.ANY)
        vmem_spec = pl.BlockSpec(memory_space=pltpu.VMEM)
        dma = pltpu.SemaphoreType.DMA
        out = pl.pallas_call(
            functools.partial(decode_kernel, cfg),
            out_shape=jax.ShapeDtypeStruct((1, model_dim), BF16),
            in_specs=[any_spec] * 11,
            out_specs=vmem_spec,
            scratch_shapes=[
                pltpu.VMEM((batch, kv_rows, LANES), BF16),
                pltpu.VMEM((batch, kv_rows, LANES), BF16),
                pltpu.VMEM((model_dim, width), BF16),
                pltpu.VMEM((model_dim // 512, width, 512), BF16),
                pltpu.VMEM((model_dim, tiles_max * LANES), BF16),
                pltpu.VMEM((model_dim, tiles_max * LANES), BF16),
                pltpu.VMEM((tiles_max * LANES, model_dim), BF16),
                pltpu.VMEM((1, model_dim), BF16),
                pltpu.VMEM((n_md, LANES), BF16),
                pltpu.VMEM((n_md, LANES), BF16),
                pltpu.VMEM((4, sel_blocks.shape[2], batch), jnp.int32),
                pltpu.VMEM((2, 2, batch, LANES), F32),
                pltpu.VMEM((16, model_dim), BF16),
                pltpu.VMEM((16, width // 2), BF16),
                pltpu.VMEM((16, LANES), BF16),
                pltpu.VMEM((batch, 16, LANES), BF16),
                pltpu.VMEM((batch * 16, kv_rows), F32),
                pltpu.VMEM((batch * 16, kv_rows), BF16),
                pltpu.VMEM((batch, 16, LANES), F32),
                pltpu.VMEM((batch, 16, LANES), F32),
                pltpu.VMEM((LANES, LANES), F32),
                pltpu.VMEM((pad_md, LANES), F32),
                pltpu.VMEM((pad_md, LANES), F32),
                pltpu.VMEM((members, pad_md, LANES), BF16),
                pltpu.VMEM((members, n_md, LANES), F32),
                pltpu.VMEM((members, n_md, LANES), F32),
                pltpu.VMEM((n_md, LANES), F32),
                pltpu.VMEM((n_md, LANES), F32),
                dma((4,)), dma((-(-width // 512),)), dma((2,)), dma((model_dim // 512,)), dma((3,)),
                dma, dma((4,)), dma, dma((2,)), dma, dma, dma, dma, dma, dma((2,)), dma((2,)), dma((2,)),
            ],
            compiler_params=pltpu.CompilerParams(
                collective_id=0, has_side_effects=True, vmem_limit_bytes=54 * 1024 * 1024),
            name="decode_step",
        )(hidden, g_attn.reshape(n_md, LANES), g_mlp.reshape(n_md, LANES), sel_blocks.transpose(1, 2, 0), k_rows, v_rows, w_q, w_o, w_gate, w_up, w_down)
        return out

    cache_spec = P("data", "seq", "model", None)
    in_specs = (P(("data", "seq"), None), cache_spec, cache_spec, P("data", None, None), P(None), P(None), P(None, None), P(None, None), P(None, "model"), P(None, "model"), P("model", None))
    return jax.shard_map(device_step, mesh=mesh, in_specs=in_specs, out_specs=P(("data", "seq"), None), check_vma=False)
```

```python
import functools

import jax
import jax.numpy as jnp
from jax import lax
from jax.experimental import pallas as pl
from jax.experimental.pallas import tpu as pltpu
from jax.sharding import PartitionSpec as P

MESH = pl.DeviceIdType.MESH
BLOCK_LEN = 64
NORM_EPS = 1e-5
LANES = 128
NEG_INF = float("-inf")
F32 = jnp.float32
BF16 = jnp.bfloat16


def row_iota(shape):
    return lax.broadcasted_iota(jnp.int32, shape, 0)


def torus_dims(seq_devs):
    side = round(seq_devs ** (1 / 3))
    return (side, side, side)


def mlp_box(dims):
    return (2, 2, dims[2]) if dims[2] > 2 else (1, 2, 2)


def box_rows(dims):
    box = mlp_box(dims)
    spans = [range(0, n, m) for n, m in zip(dims, box)]
    rows = []
    for corner in [(z, y, x) for z in spans[0] for y in spans[1] for x in spans[2]]:
        places = [(a, b, c) for a in range(box[0]) for b in range(box[1]) for c in range(box[2])]
        cells = [[p + q for p, q in zip(corner, place)] for place in places]
        rows.append([(z * dims[1] + y) * dims[2] + x for z, y, x in cells])
    return rows


def push_offsets(dims):
    offsets = [(a, b, c) for a in range(dims[0]) for b in range(dims[1]) for c in range(dims[2])]
    return sorted(offsets, key=lambda o: (-sum(min(d, n - d) for d, n in zip(o, dims)), o))


def decode_kernel(
    cfg,
    hid_hbm, ga_hbm, gm_hbm, sel_hbm, k_hbm, v_hbm, wq_hbm, wo_hbm, wg_hbm, wu_hbm, wd_hbm,
    out_ref,
    k_buf, v_buf, wq_buf, wo_buf, wg_buf, wu_buf, wd_buf,
    hid_ref, ga_ref, gm_ref, sel_ref, hit_buf, lhs_buf, olhs_buf,
    q_out, q_all, s_buf, p_buf, part_out, part_in, stat_buf,
    pair_out, pair_in, h2_all, mlp_out, mlp_in, fin_out, fin_in,
    small_sem, wq_sem, kv_sem, wo_sem, mlp_sem,
    q_send, q_recv, part_send, part_recv, pair_send, pair_recv, h2_send, h2_recv,
    red_send, red_recv, fin_send, fin_recv,
):
    seqs, n_md, tiles_ffn, tiles_max = cfg
    dims = torus_dims(seqs)
    box = mlp_box(dims)
    members = box[0] * box[1] * box[2]
    push_order, groups = push_offsets(dims), box_rows(dims)
    core = lax.axis_index("model")
    other = 1 - core
    me = lax.axis_index("seq")
    place = (me // (dims[1] * dims[2]), (me // dims[2]) % dims[1], me % dims[2])

    def seq_at(offset):
        z, y, x = (lax.rem(p + o, n) if o else p for p, o, n in zip(place, offset, dims))
        return (z * dims[1] + y) * dims[2] + x

    inner = tuple(p % n for p, n in zip(place, box))
    my_slot = (inner[0] * box[1] + inner[1]) * box[2] + inner[2]

    def member_at(offset):
        z, y, x = (lax.rem(p + o, n) if o else p for p, o, n in zip(inner, offset, box))
        slot = (z * box[1] + y) * box[2] + x
        whole = [p - i + v for p, i, v in zip(place, inner, (z, y, x))]
        return slot, (whole[0] * dims[1] + whole[1]) * dims[2] + whole[2]

    def box_hops(o):
        return sum(min(d, n - d) for d, n in zip(o, box))

    my_box = place[0] // box[0]
    for p, n, m in zip(place[1:], dims[1:], box[1:]):
        my_box = my_box * (n // m) + p // m

    def row_in_box(k, j):
        first = groups[k][0]
        z, y, x = j // (box[1] * box[2]), (j // box[2]) % box[1], j % box[2]
        return first + (z * dims[1] + y) * dims[2] + x

    box_offsets = [(a, b, c) for a in range(box[0]) for b in range(box[1]) for c in range(box[2])]
    box_far_first = sorted(box_offsets, key=lambda o: (-box_hops(o), o))

    heads = 14
    width = heads * LANES
    q_chunks = -(-wq_buf.shape[1] // 512)
    o_chunks = wo_buf.shape[0]
    model_dim = n_md * LANES
    pad_md = pair_out.shape[0]
    k_parts = 4
    part_rows = model_dim // k_parts

    wq_cols = [(c, min(512, width - c)) for c in range(0, width, 512)]

    def wq_start(n):
        at, size = wq_cols[n]
        cols = pl.ds(pl.multiple_of(other * width + at, LANES), size)
        for part in range(k_parts):
            rows = pl.ds(part * part_rows, part_rows)
            pltpu.make_async_copy(wq_hbm.at[rows, cols], wq_buf.at[rows, pl.ds(at, size)], wq_sem.at[n]).start()

    def wq_wait(n):
        at, size = wq_cols[n]
        done = wq_buf.at[:, pl.ds(at, size)]
        pltpu.make_async_copy(done, done, wq_sem.at[n]).wait()

    runs = []
    for k, rows in enumerate(groups):
        for row in rows:
            if runs and runs[-1][0] == k and runs[-1][1] + runs[-1][2] == row:
                runs[-1][2] += 1
            else:
                runs.append([k, row, 1])

    def kv_start(which, group):
        src, dst = ((k_hbm, k_buf), (v_hbm, v_buf))[which]
        for k, row, count in runs:
            if k == group:
                rows = pl.ds(row, count)
                pltpu.make_async_copy(src.at[rows], dst.at[rows], kv_sem.at[which, k]).start()

    def kv_wait(which, k):
        done = (k_buf, v_buf)[which].at[pl.ds(0, len(groups[k]))]
        pltpu.make_async_copy(done, done, kv_sem.at[which, k]).wait()

    def wo_copy(n):
        rows = pl.ds(pl.multiple_of(other * width, LANES), width)
        return pltpu.make_async_copy(wo_hbm.at[rows, pl.ds(n * 512, 512)], wo_buf.at[n], wo_sem.at[n])

    first_tile = (tiles_ffn * my_slot) // members
    my_tiles = (tiles_ffn * (my_slot + 1)) // members - first_tile
    ffn_cols = pl.ds(pl.multiple_of(first_tile * LANES, LANES), tiles_max * LANES)

    def up_start(which):
        src, dst = ((wg_hbm, wg_buf), (wu_hbm, wu_buf))[which]
        for part in range(k_parts):
            rows = pl.ds(part * part_rows, part_rows)
            pltpu.make_async_copy(src.at[rows, ffn_cols], dst.at[rows], mlp_sem.at[which]).start()

    def up_wait(which):
        dst = (wg_buf, wu_buf)[which]
        pltpu.make_async_copy(dst, dst, mlp_sem.at[which]).wait()

    wd_copy = pltpu.make_async_copy(wd_hbm.at[ffn_cols, :], wd_buf, mlp_sem.at[2])

    smalls = [
        pltpu.make_async_copy(src, dst, small_sem.at[n])
        for n, (src, dst) in enumerate(((hid_hbm, hid_ref), (ga_hbm, ga_ref), (gm_hbm, gm_ref), (sel_hbm, sel_ref)))
    ]
    for copy in smalls[:2]:
        copy.start()

    barrier = pltpu.get_barrier_semaphore()

    def greet(d):
        pl.semaphore_signal(barrier, inc=1, device_id={"model": other, "seq": d}, device_id_type=MESH)

    early = seqs // 4
    pl.loop(0, early)(greet)
    for n in range(q_chunks):
        wq_start(n)
    for copy in smalls[2:]:
        copy.start()
    pl.loop(early, seqs)(greet)

    smalls[0].wait()
    smalls[1].wait()
    rows8 = row_iota((8, LANES))
    rows16 = row_iota((16, LANES))
    lane16 = lax.broadcasted_iota(jnp.int32, (16, LANES), 1)
    hid_parts = [jnp.zeros((8, LANES), F32) for _ in range(pad_md // 8)]
    for n in range(n_md):
        piece = jnp.broadcast_to(hid_ref[:, n * LANES:(n + 1) * LANES].astype(F32), (8, LANES))
        hid_parts[n // 8] = jnp.where(rows8 == n % 8, piece, hid_parts[n // 8])
    hid = jnp.concatenate(hid_parts, axis=0)
    fill = jnp.zeros((pad_md - n_md, LANES), F32)

    def norm(x, gain_ref):
        inv = lax.rsqrt(jnp.sum(x * x, keepdims=True) / model_dim + NORM_EPS)
        return (x * inv * jnp.concatenate([gain_ref[...].astype(F32), fill], axis=0)).astype(BF16)

    h_attn = norm(hid, ga_ref).astype(F32)
    for n in range(n_md):
        lhs_buf[:, n * LANES:(n + 1) * LANES] = jnp.broadcast_to(h_attn[n:n + 1, :], (16, LANES)).astype(BF16)

    q_tile = jnp.zeros((16, LANES), F32)
    head = 0
    for n in range(q_chunks):
        wq_wait(n)
        if n == q_chunks - 2:
            kv_start(0, 0)
            kv_start(1, 0)
        if n == q_chunks - 1:
            for k in range(1, len(groups)):
                kv_start(0, k)
                kv_start(1, k)
        at, size = wq_cols[n]
        span = 512 if size == 512 else LANES
        for low in range(at, at + size, span):
            acc = jnp.dot(lhs_buf[...], wq_buf[:, low:low + span], preferred_element_type=F32) * (LANES ** -0.5)
            for t in range(span // LANES):
                q_tile = jnp.where(rows16 == head + head // 7, acc[:, t * LANES:(t + 1) * LANES], q_tile)
                head += 1
    q_out[...] = q_tile.astype(BF16)

    pl.semaphore_wait(barrier, seqs)

    for offset in push_order:
        pltpu.make_async_remote_copy(
            src_ref=q_out, dst_ref=q_all.at[me], send_sem=q_send, recv_sem=q_recv.at[my_box],
            device_id={"model": other, "seq": seq_at(offset)}, device_id_type=MESH).start()
    for n in range(o_chunks):
        wo_copy(n).start()
    up_start(0)
    up_start(1)
    wd_copy.start()

    stat_buf[...] = jnp.zeros((LANES, LANES), F32)
    smalls[3].wait()
    for j in range(2):
        found = [
            jnp.max(jnp.where(sel_ref[g] == me * 2 + j, 1.0, 0.0), axis=0, keepdims=True)
            for g in range(4)
        ]
        for g in range(2):
            mine = jnp.where(core == 0, found[g], found[2 + g])
            column = jnp.broadcast_to(mine, (8, seqs)).T[:, 0:1]
            hit_buf[j, g] = jnp.broadcast_to(jnp.where(column > 0.5, 0.0, NEG_INF), (seqs, LANES))

    parity = ((lane16 % 2) == jnp.where(rows16 < 8, 0, 1)) & (rows16 % 8 != 7)
    order = [(k, i, row) for k, group in enumerate(groups) for i, row in enumerate(group)]
    tops = {}
    stats = {k: [jnp.zeros((16, LANES), F32)] * 2 for k in range(len(groups))}
    gap = 5
    drains = ()
    slots = [None]
    for n, item in enumerate(order):
        if item[1] == 0 and item[0] in drains:
            slots += [None] * (3 * gap)
        slots.append((n,) + item)
    slots += [None] * (3 * gap)

    def spot(n):
        return slice(n * 16, (n + 1) * 16)

    def push_half(row, half):
        tile = pl.ds(half * 8, 8)
        pltpu.make_async_remote_copy(
            src_ref=part_out.at[row, tile], dst_ref=part_in.at[me, tile], send_sem=part_send, recv_sem=part_recv.at[half],
            device_id={"model": other, "seq": row}, device_id_type=MESH).start()

    def push_box(k, half):
        for i in range(members):
            push_half(row_in_box(k, lax.rem(my_slot + i, members)), half)

    def score_stage(n, k, i, row):
        if i == 0:
            arrived = q_all.at[pl.ds(0, len(groups[k]))]
            pltpu.make_async_copy(arrived, arrived, q_recv.at[k]).wait()
            kv_wait(0, k)
            kv_wait(1, k)
        scores = lax.dot_general(q_all[row], k_buf[row], (((1,), (1,)), ((), ())), preferred_element_type=F32)
        for j in range(2):
            hit_0 = jnp.broadcast_to(hit_buf[j, 0, row:row + 1, :], (16, LANES))
            hit_1 = jnp.broadcast_to(hit_buf[j, 1, row:row + 1, :], (16, LANES))
            bias = jnp.where(parity, jnp.where(rows16 < 8, hit_0, hit_1), NEG_INF)
            s_buf[spot(n), j * LANES:(j + 1) * LANES] = scores[:, j * LANES:(j + 1) * LANES] + bias

    def top_stage(n, k, i, row):
        tops[n] = jnp.max(s_buf[spot(n), :], axis=1, keepdims=True)

    def exp_stage(n, k, i, row):
        top = tops.pop(n)
        safe = jnp.where(top == NEG_INF, 0.0, top)
        exps = jnp.exp(s_buf[spot(n), :] - safe)
        p_buf[spot(n), :] = exps.astype(BF16)
        total = jnp.sum(exps, axis=1, keepdims=True)
        stats[k] = [jnp.where(lane16 == i, v, old) for v, old in zip((top, total), stats[k])]

    def value_stage(n, k, i, row):
        part_out[row] = jnp.dot(p_buf[spot(n), :], v_buf[row], preferred_element_type=F32)
        if i == len(groups[k]) - 1:
            stats_t = jnp.concatenate(stats[k], axis=0).T
            rows = [item[2] for item in order if item[0] == k]
            for m, to in enumerate(rows):
                part_out[to, 7:8, 0:32] = stats_t[m:m + 1, :]
                part_out[to, 15:16, 0:32] = stats_t[m:m + 1, :]
            push_box(k, 0)
            if k > 0:
                push_box(k - 1, 1)

    for t in range(len(slots)):
        for lag, stage in ((0, score_stage), (gap, top_stage), (2 * gap, exp_stage), (3 * gap, value_stage)):
            if t >= lag and slots[t - lag] is not None:
                stage(*slots[t - lag])
    push_box(len(groups) - 1, 1)

    proj = [jnp.zeros((8, LANES), F32) for _ in range(pad_md // 8)]
    half_width = width // 2
    for half in range(2):
        tile = slice(half * 8, half * 8 + 8)
        landed = part_in.at[:, pl.ds(half * 8, 8)]
        pltpu.make_async_copy(landed, landed, part_recv.at[half]).wait()
        if half == 0:
            for i in range(seqs):
                stat_buf[i:i + 1, :] = part_in[i, 7:8, :]
            stat_t = stat_buf[...].T
            real = lax.broadcasted_iota(jnp.int32, (16, LANES), 1) < seqs
            top = jnp.where(real, stat_t[0:16, :], NEG_INF)
            scales = jnp.exp(top - jnp.max(top, axis=1, keepdims=True))
            mass = jnp.where(real, stat_t[16:32, :], 0.0)
            denoms = jnp.sum(scales * mass, axis=1, keepdims=True)
        scale, denom = scales[tile, :], denoms[tile, :]
        sums = [jnp.zeros((8, LANES), F32) for _ in range(4)]
        for i in range(seqs):
            sums[i % 4] = sums[i % 4] + scale[:, i:i + 1] * part_in[i, tile, :]
        attn = (((sums[0] + sums[1]) + (sums[2] + sums[3])) / denom).astype(BF16).astype(F32)
        for r in range(7):
            olhs_buf[:, r * LANES:(r + 1) * LANES] = jnp.broadcast_to(attn[r:r + 1, :], (16, LANES)).astype(BF16)
        if half == 0:
            for n in range(o_chunks):
                wo_copy(n).wait()
        for n in range(o_chunks):
            acc = jnp.dot(olhs_buf[...], wo_buf[n, half * half_width:(half + 1) * half_width, :], preferred_element_type=F32)
            for t in range(4):
                r = 4 * n + t
                here = jnp.where(rows8 == r % 8, acc[0:8, t * LANES:(t + 1) * LANES], 0.0)
                proj[r // 8] = proj[r // 8] + here
    for r in range(pad_md // 8):
        pair_out[r * 8:(r + 1) * 8, :] = proj[r]
    pair = pltpu.make_async_remote_copy(
        src_ref=pair_out, dst_ref=pair_in, send_sem=pair_send, recv_sem=pair_recv,
        device_id={"model": other}, device_id_type=MESH)
    pair.start()
    pair.wait()
    smalls[2].wait()
    resid = (hid + (pair_out[...] + pair_in[...])).astype(BF16).astype(F32)
    h2_all[my_slot] = norm(resid, gm_ref)

    for offset in box_far_first:
        if any(offset):
            pltpu.make_async_remote_copy(
                src_ref=h2_all.at[my_slot], dst_ref=h2_all.at[my_slot], send_sem=h2_send, recv_sem=h2_recv,
                device_id={"model": other, "seq": member_at(offset)[1]}, device_id_type=MESH).start()
    gone = h2_all.at[pl.ds(0, members - 1)]
    pltpu.make_async_copy(gone, gone, h2_recv).wait()
    rows = [h2_all[i].astype(F32) for i in range(members)]
    for n in range(n_md):
        tile = jnp.zeros((16, LANES), F32)
        for i in range(members):
            tile = jnp.where(rows16 == i, jnp.broadcast_to(rows[i][n:n + 1, :], (16, LANES)), tile)
        lhs_buf[:, n * LANES:(n + 1) * LANES] = tile.astype(BF16)

    up_wait(0)
    up_wait(1)
    wd_copy.wait()
    gate = jnp.dot(lhs_buf[...], wg_buf[...], preferred_element_type=F32).astype(BF16).astype(F32)
    up = jnp.dot(lhs_buf[...], wu_buf[...], preferred_element_type=F32).astype(BF16).astype(F32)
    act = jax.nn.silu(gate) * up
    cols = lax.broadcasted_iota(jnp.int32, act.shape, 1)
    act = jnp.where(cols < my_tiles * LANES, act, 0.0).astype(BF16)
    cut = min(16, n_md // 2 // 4 * 4) if n_md > 4 else 0
    pieces = [(0, cut), (cut, n_md)] if cut else [(0, n_md)]
    homes = [member_at(offset) for offset in box_far_first]

    def down(n):
        return jnp.dot(act, wd_buf[:, n * 512:(n + 1) * 512], preferred_element_type=F32)

    ahead = down(0)
    for piece, (low, high) in enumerate(pieces):
        for n in range(low // 4, high // 4):
            acc = ahead
            if n + 1 < o_chunks:
                ahead = down(n + 1)
            for t in range(4):
                for i in range(members):
                    mlp_out[i, 4 * n + t:4 * n + t + 1, :] = acc[i:i + 1, t * LANES:(t + 1) * LANES]
        for slot, home in homes:
            tile = pl.ds(low, high - low)
            pltpu.make_async_remote_copy(
                src_ref=mlp_out.at[slot, tile], dst_ref=mlp_in.at[my_slot, tile], send_sem=red_send, recv_sem=red_recv.at[piece],
                device_id={"model": other, "seq": home}, device_id_type=MESH).start()

    finals = []
    for piece, (low, high) in enumerate(pieces):
        tile = pl.ds(low, high - low)
        landed = mlp_in.at[:, tile]
        pltpu.make_async_copy(landed, landed, red_recv.at[piece]).wait()
        total = mlp_in[0, low:high, :]
        for i in range(1, members):
            total = total + mlp_in[i, low:high, :]
        fin_out[low:high, :] = total
        fin = pltpu.make_async_remote_copy(
            src_ref=fin_out.at[tile], dst_ref=fin_in.at[tile], send_sem=fin_send.at[piece], recv_sem=fin_recv.at[piece],
            device_id={"model": other}, device_id_type=MESH)
        fin.start()
        finals.append(fin)
    for fin in finals:
        fin.wait()
    result = resid[0:n_md, :] + (fin_out[...] + fin_in[...])
    for n in range(n_md):
        out_ref[:, n * LANES:(n + 1) * LANES] = result[n:n + 1, :].astype(BF16)

    pltpu.make_async_copy(q_all, q_all, q_send).wait()
    pltpu.make_async_copy(part_in, part_in, part_send).wait()
    pltpu.make_async_copy(gone, gone, h2_send).wait()
    pltpu.make_async_copy(mlp_in, mlp_in, red_send).wait()


def solution(mesh):
    model_devs = mesh.shape["model"]
    seq_devs = mesh.shape["seq"]

    def device_step(hidden, k_cache, v_cache, sel_blocks, g_attn, g_mlp, w_q, w_o, w_gate, w_up, w_down):
        model_dim = hidden.shape[1]
        batch, tokens, kv_local, head_dim = k_cache.shape
        n_md = model_dim // LANES
        pad_md = -(-n_md // 16) * 16
        dims = torus_dims(seq_devs)
        box = mlp_box(dims)
        members = box[0] * box[1] * box[2]
        tiles_ffn = w_gate.shape[1] // LANES
        tiles_max = -(-tiles_ffn // members)
        width = w_q.shape[1] // model_devs
        kv_rows = tokens * kv_local
        k_rows = k_cache.reshape(batch, kv_rows, head_dim)
        v_rows = v_cache.reshape(batch, kv_rows, head_dim)
        cfg = (seq_devs, n_md, tiles_ffn, tiles_max)
        any_spec = pl.BlockSpec(memory_space=pl.ANY)
        vmem_spec = pl.BlockSpec(memory_space=pltpu.VMEM)
        dma = pltpu.SemaphoreType.DMA
        out = pl.pallas_call(
            functools.partial(decode_kernel, cfg),
            out_shape=jax.ShapeDtypeStruct((1, model_dim), BF16),
            in_specs=[any_spec] * 11,
            out_specs=vmem_spec,
            scratch_shapes=[
                pltpu.VMEM((batch, kv_rows, LANES), BF16),
                pltpu.VMEM((batch, kv_rows, LANES), BF16),
                pltpu.VMEM((model_dim, width), BF16),
                pltpu.VMEM((model_dim // 512, width, 512), BF16),
                pltpu.VMEM((model_dim, tiles_max * LANES), BF16),
                pltpu.VMEM((model_dim, tiles_max * LANES), BF16),
                pltpu.VMEM((tiles_max * LANES, model_dim), BF16),
                pltpu.VMEM((1, model_dim), BF16),
                pltpu.VMEM((n_md, LANES), BF16),
                pltpu.VMEM((n_md, LANES), BF16),
                pltpu.VMEM((4, sel_blocks.shape[2], batch), jnp.int32),
                pltpu.VMEM((2, 2, batch, LANES), F32),
                pltpu.VMEM((16, model_dim), BF16),
                pltpu.VMEM((16, width // 2), BF16),
                pltpu.VMEM((16, LANES), BF16),
                pltpu.VMEM((batch, 16, LANES), BF16),
                pltpu.VMEM((batch * 16, kv_rows), F32),
                pltpu.VMEM((batch * 16, kv_rows), BF16),
                pltpu.VMEM((batch, 16, LANES), F32),
                pltpu.VMEM((batch, 16, LANES), F32),
                pltpu.VMEM((LANES, LANES), F32),
                pltpu.VMEM((pad_md, LANES), F32),
                pltpu.VMEM((pad_md, LANES), F32),
                pltpu.VMEM((members, pad_md, LANES), BF16),
                pltpu.VMEM((members, n_md, LANES), F32),
                pltpu.VMEM((members, n_md, LANES), F32),
                pltpu.VMEM((n_md, LANES), F32),
                pltpu.VMEM((n_md, LANES), F32),
                dma((4,)), dma((-(-width // 512),)), dma((2, 5)), dma((model_dim // 512,)), dma((3,)),
                dma, dma((5,)), dma, dma((2,)), dma, dma, dma, dma, dma, dma((2,)), dma((2,)), dma((2,)),
            ],
            compiler_params=pltpu.CompilerParams(
                collective_id=0, has_side_effects=True, vmem_limit_bytes=54 * 1024 * 1024),
            name="decode_step",
        )(hidden, g_attn.reshape(n_md, LANES), g_mlp.reshape(n_md, LANES), sel_blocks.transpose(1, 2, 0), k_rows, v_rows, w_q, w_o, w_gate, w_up, w_down)
        return out

    cache_spec = P("data", "seq", "model", None)
    in_specs = (P(("data", "seq"), None), cache_spec, cache_spec, P("data", None, None), P(None), P(None), P(None, None), P(None, None), P(None, "model"), P(None, "model"), P("model", None))
    return jax.shard_map(device_step, mesh=mesh, in_specs=in_specs, out_specs=P(("data", "seq"), None), check_vma=False)
```

```python
import functools

import jax
import jax.numpy as jnp
from jax import lax
from jax.experimental import pallas as pl
from jax.experimental.pallas import tpu as pltpu
from jax.sharding import PartitionSpec as P

MESH = pl.DeviceIdType.MESH
BLOCK_LEN = 64
NORM_EPS = 1e-5
LANES = 128
NEG_INF = float("-inf")
F32 = jnp.float32
BF16 = jnp.bfloat16


def row_iota(shape):
    return lax.broadcasted_iota(jnp.int32, shape, 0)


def torus_dims(seq_devs):
    side = round(seq_devs ** (1 / 3))
    return (side, side, side)


def mlp_box(dims):
    return (2, 2, dims[2]) if dims[2] > 2 else (1, 2, 2)


def box_rows(dims):
    box = mlp_box(dims)
    spans = [range(0, n, m) for n, m in zip(dims, box)]
    rows = []
    for corner in [(z, y, x) for z in spans[0] for y in spans[1] for x in spans[2]]:
        places = [(a, b, c) for a in range(box[0]) for b in range(box[1]) for c in range(box[2])]
        cells = [[p + q for p, q in zip(corner, place)] for place in places]
        rows.append([(z * dims[1] + y) * dims[2] + x for z, y, x in cells])
    return rows


def push_offsets(dims):
    offsets = [(a, b, c) for a in range(dims[0]) for b in range(dims[1]) for c in range(dims[2])]
    return sorted(offsets, key=lambda o: (-sum(min(d, n - d) for d, n in zip(o, dims)), o))


def decode_kernel(
    cfg,
    hid_hbm, ga_hbm, gm_hbm, sel_hbm, k_hbm, v_hbm, wq_hbm, wo_hbm, wg_hbm, wu_hbm, wd_hbm,
    out_ref,
    k_buf, v_buf, wq_buf, wo_buf, wg_buf, wu_buf, wd_buf,
    hid_ref, ga_ref, gm_ref, sel_ref, hit_buf, lhs_buf, olhs_buf,
    q_out, q_all, s_buf, p_buf, part_out, part_in, stat_buf,
    pair_out, pair_in, h2_all, mlp_out, mlp_in, fin_out, fin_in,
    small_sem, wq_sem, kv_sem, wo_sem, mlp_sem,
    q_send, q_recv, part_send, part_recv, pair_send, pair_recv, h2_send, h2_recv,
    red_send, red_recv, fin_send, fin_recv,
):
    seqs, n_md, tiles_ffn, tiles_max = cfg
    dims = torus_dims(seqs)
    box = mlp_box(dims)
    members = box[0] * box[1] * box[2]
    push_order, groups = push_offsets(dims), box_rows(dims)
    core = lax.axis_index("model")
    other = 1 - core
    me = lax.axis_index("seq")
    place = (me // (dims[1] * dims[2]), (me // dims[2]) % dims[1], me % dims[2])

    def seq_at(offset):
        z, y, x = (lax.rem(p + o, n) if o else p for p, o, n in zip(place, offset, dims))
        return (z * dims[1] + y) * dims[2] + x

    inner = tuple(p % n for p, n in zip(place, box))
    my_slot = (inner[0] * box[1] + inner[1]) * box[2] + inner[2]

    def member_at(offset):
        z, y, x = (lax.rem(p + o, n) if o else p for p, o, n in zip(inner, offset, box))
        slot = (z * box[1] + y) * box[2] + x
        whole = [p - i + v for p, i, v in zip(place, inner, (z, y, x))]
        return slot, (whole[0] * dims[1] + whole[1]) * dims[2] + whole[2]

    def box_hops(o):
        return sum(min(d, n - d) for d, n in zip(o, box))

    my_box = place[0] // box[0]
    for p, n, m in zip(place[1:], dims[1:], box[1:]):
        my_box = my_box * (n // m) + p // m

    def row_in_box(k, j):
        first = groups[k][0]
        z, y, x = j // (box[1] * box[2]), (j // box[2]) % box[1], j % box[2]
        return first + (z * dims[1] + y) * dims[2] + x

    box_offsets = [(a, b, c) for a in range(box[0]) for b in range(box[1]) for c in range(box[2])]
    box_far_first = sorted(box_offsets, key=lambda o: (-box_hops(o), o))

    heads = 14
    width = heads * LANES
    q_chunks = -(-wq_buf.shape[1] // 512)
    o_chunks = wo_buf.shape[0]
    model_dim = n_md * LANES
    pad_md = pair_out.shape[0]
    k_parts = 4
    part_rows = model_dim // k_parts

    wq_cols = [(c, min(512, width - c)) for c in range(0, width, 512)]

    def wq_start(n):
        at, size = wq_cols[n]
        cols = pl.ds(pl.multiple_of(other * width + at, LANES), size)
        for part in range(k_parts):
            rows = pl.ds(part * part_rows, part_rows)
            pltpu.make_async_copy(wq_hbm.at[rows, cols], wq_buf.at[rows, pl.ds(at, size)], wq_sem.at[n]).start()

    def wq_wait(n):
        at, size = wq_cols[n]
        done = wq_buf.at[:, pl.ds(at, size)]
        pltpu.make_async_copy(done, done, wq_sem.at[n]).wait()

    runs = []
    for k, rows in enumerate(groups):
        for row in rows:
            if runs and runs[-1][0] == k and runs[-1][1] + runs[-1][2] == row:
                runs[-1][2] += 1
            else:
                runs.append([k, row, 1])

    def kv_start(which, group):
        src, dst = ((k_hbm, k_buf), (v_hbm, v_buf))[which]
        for k, row, count in runs:
            if k == group:
                rows = pl.ds(row, count)
                pltpu.make_async_copy(src.at[rows], dst.at[rows], kv_sem.at[which, k]).start()

    def kv_wait(which, k):
        done = (k_buf, v_buf)[which].at[pl.ds(0, len(groups[k]))]
        pltpu.make_async_copy(done, done, kv_sem.at[which, k]).wait()

    def wo_copy(n):
        rows = pl.ds(pl.multiple_of(other * width, LANES), width)
        return pltpu.make_async_copy(wo_hbm.at[rows, pl.ds(n * 512, 512)], wo_buf.at[n], wo_sem.at[n])

    first_tile = (tiles_ffn * my_slot) // members
    my_tiles = (tiles_ffn * (my_slot + 1)) // members - first_tile
    ffn_cols = pl.ds(pl.multiple_of(first_tile * LANES, LANES), tiles_max * LANES)

    def up_start(which):
        src, dst = ((wg_hbm, wg_buf), (wu_hbm, wu_buf))[which]
        for part in range(k_parts):
            rows = pl.ds(part * part_rows, part_rows)
            pltpu.make_async_copy(src.at[rows, ffn_cols], dst.at[rows], mlp_sem.at[which]).start()

    def up_wait(which):
        dst = (wg_buf, wu_buf)[which]
        pltpu.make_async_copy(dst, dst, mlp_sem.at[which]).wait()

    wd_copy = pltpu.make_async_copy(wd_hbm.at[ffn_cols, :], wd_buf, mlp_sem.at[2])

    smalls = [
        pltpu.make_async_copy(src, dst, small_sem.at[n])
        for n, (src, dst) in enumerate(((hid_hbm, hid_ref), (ga_hbm, ga_ref), (gm_hbm, gm_ref), (sel_hbm, sel_ref)))
    ]
    for copy in smalls[:2]:
        copy.start()

    barrier = pltpu.get_barrier_semaphore()

    def greet(d):
        pl.semaphore_signal(barrier, inc=1, device_id={"model": other, "seq": d}, device_id_type=MESH)

    early = seqs // 4
    pl.loop(0, early)(greet)
    for n in range(q_chunks):
        wq_start(n)
    for copy in smalls[2:]:
        copy.start()
    pl.loop(early, seqs)(greet)

    smalls[0].wait()
    smalls[1].wait()
    rows8 = row_iota((8, LANES))
    rows16 = row_iota((16, LANES))
    lane16 = lax.broadcasted_iota(jnp.int32, (16, LANES), 1)
    hid_parts = [jnp.zeros((8, LANES), F32) for _ in range(pad_md // 8)]
    for n in range(n_md):
        piece = jnp.broadcast_to(hid_ref[:, n * LANES:(n + 1) * LANES].astype(F32), (8, LANES))
        hid_parts[n // 8] = jnp.where(rows8 == n % 8, piece, hid_parts[n // 8])
    hid = jnp.concatenate(hid_parts, axis=0)
    fill = jnp.zeros((pad_md - n_md, LANES), F32)

    def norm(x, gain_ref):
        inv = lax.rsqrt(jnp.sum(x * x, keepdims=True) / model_dim + NORM_EPS)
        return (x * inv * jnp.concatenate([gain_ref[...].astype(F32), fill], axis=0)).astype(BF16)

    h_attn = norm(hid, ga_ref).astype(F32)
    for n in range(n_md):
        lhs_buf[:, n * LANES:(n + 1) * LANES] = jnp.broadcast_to(h_attn[n:n + 1, :], (16, LANES)).astype(BF16)

    q_tile = jnp.zeros((16, LANES), F32)
    head = 0
    for n in range(q_chunks):
        wq_wait(n)
        if n == q_chunks - 2:
            kv_start(0, 0)
            kv_start(1, 0)
        if n == q_chunks - 1:
            for k in range(1, len(groups)):
                kv_start(0, k)
                kv_start(1, k)
        at, size = wq_cols[n]
        span = 512 if size == 512 else LANES
        for low in range(at, at + size, span):
            acc = jnp.dot(lhs_buf[...], wq_buf[:, low:low + span], preferred_element_type=F32) * (LANES ** -0.5)
            for t in range(span // LANES):
                q_tile = jnp.where(rows16 == head + head // 7, acc[:, t * LANES:(t + 1) * LANES], q_tile)
                head += 1
    q_out[...] = q_tile.astype(BF16)

    pl.semaphore_wait(barrier, seqs)

    for offset in push_order:
        pltpu.make_async_remote_copy(
            src_ref=q_out, dst_ref=q_all.at[me], send_sem=q_send, recv_sem=q_recv.at[my_box],
            device_id={"model": other, "seq": seq_at(offset)}, device_id_type=MESH).start()
    for n in range(o_chunks):
        wo_copy(n).start()
    up_start(0)
    up_start(1)
    wd_copy.start()

    stat_buf[...] = jnp.zeros((LANES, LANES), F32)
    smalls[3].wait()
    for j in range(2):
        found = [
            jnp.max(jnp.where(sel_ref[g] == me * 2 + j, 1.0, 0.0), axis=0, keepdims=True)
            for g in range(4)
        ]
        for g in range(2):
            mine = jnp.where(core == 0, found[g], found[2 + g])
            column = jnp.broadcast_to(mine, (8, seqs)).T[:, 0:1]
            hit_buf[j, g] = jnp.broadcast_to(jnp.where(column > 0.5, 0.0, NEG_INF), (seqs, LANES))

    parity = ((lane16 % 2) == jnp.where(rows16 < 8, 0, 1)) & (rows16 % 8 != 7)
    order = [(k, i, row) for k, group in enumerate(groups) for i, row in enumerate(group)]
    tops = {}
    stats = {k: [jnp.zeros((16, LANES), F32)] * 2 for k in range(len(groups))}
    gap = 4
    drains = (1,)
    slots = [None]
    for n, item in enumerate(order):
        if item[1] == 0 and item[0] in drains:
            slots += [None] * (3 * gap)
        slots.append((n,) + item)
    slots += [None] * (3 * gap)

    def spot(n):
        return slice(n * 16, (n + 1) * 16)

    def push_half(row, half):
        tile = pl.ds(half * 8, 8)
        pltpu.make_async_remote_copy(
            src_ref=part_out.at[row, tile], dst_ref=part_in.at[me, tile], send_sem=part_send, recv_sem=part_recv.at[half],
            device_id={"model": other, "seq": row}, device_id_type=MESH).start()

    def push_box(k, half):
        for i in range(members):
            push_half(row_in_box(k, lax.rem(my_slot + i, members)), half)

    def score_stage(n, k, i, row):
        if i == 0:
            arrived = q_all.at[pl.ds(0, len(groups[k]))]
            pltpu.make_async_copy(arrived, arrived, q_recv.at[k]).wait()
            kv_wait(0, k)
            kv_wait(1, k)
        scores = lax.dot_general(q_all[row], k_buf[row], (((1,), (1,)), ((), ())), preferred_element_type=F32)
        for j in range(2):
            hit_0 = jnp.broadcast_to(hit_buf[j, 0, row:row + 1, :], (16, LANES))
            hit_1 = jnp.broadcast_to(hit_buf[j, 1, row:row + 1, :], (16, LANES))
            bias = jnp.where(parity, jnp.where(rows16 < 8, hit_0, hit_1), NEG_INF)
            s_buf[spot(n), j * LANES:(j + 1) * LANES] = scores[:, j * LANES:(j + 1) * LANES] + bias

    def top_stage(n, k, i, row):
        tops[n] = jnp.max(s_buf[spot(n), :], axis=1, keepdims=True)

    def exp_stage(n, k, i, row):
        top = tops.pop(n)
        safe = jnp.where(top == NEG_INF, 0.0, top)
        exps = jnp.exp(s_buf[spot(n), :] - safe)
        p_buf[spot(n), :] = exps.astype(BF16)
        total = jnp.sum(exps, axis=1, keepdims=True)
        stats[k] = [jnp.where(lane16 == i, v, old) for v, old in zip((top, total), stats[k])]

    def value_stage(n, k, i, row):
        part_out[row] = jnp.dot(p_buf[spot(n), :], v_buf[row], preferred_element_type=F32)
        if i == len(groups[k]) - 1:
            stats_t = jnp.concatenate(stats[k], axis=0).T
            rows = [item[2] for item in order if item[0] == k]
            for m, to in enumerate(rows):
                part_out[to, 7:8, 0:32] = stats_t[m:m + 1, :]
                part_out[to, 15:16, 0:32] = stats_t[m:m + 1, :]
            push_box(k, 0)
            if k == 0:
                push_box(0, 1)
            if k > 1:
                push_box(k - 1, 1)

    for t in range(len(slots)):
        for lag, stage in ((0, score_stage), (gap, top_stage), (2 * gap, exp_stage), (3 * gap, value_stage)):
            if t >= lag and slots[t - lag] is not None:
                stage(*slots[t - lag])
    push_box(len(groups) - 1, 1)

    proj = [jnp.zeros((8, LANES), F32) for _ in range(pad_md // 8)]
    half_width = width // 2
    for half in range(2):
        tile = slice(half * 8, half * 8 + 8)
        landed = part_in.at[:, pl.ds(half * 8, 8)]
        pltpu.make_async_copy(landed, landed, part_recv.at[half]).wait()
        if half == 0:
            for i in range(seqs):
                stat_buf[i:i + 1, :] = part_in[i, 7:8, :]
            stat_t = stat_buf[...].T
            real = lax.broadcasted_iota(jnp.int32, (16, LANES), 1) < seqs
            top = jnp.where(real, stat_t[0:16, :], NEG_INF)
            scales = jnp.exp(top - jnp.max(top, axis=1, keepdims=True))
            mass = jnp.where(real, stat_t[16:32, :], 0.0)
            denoms = jnp.sum(scales * mass, axis=1, keepdims=True)
        scale, denom = scales[tile, :], denoms[tile, :]
        sums = [jnp.zeros((8, LANES), F32) for _ in range(4)]
        for i in range(seqs):
            sums[i % 4] = sums[i % 4] + scale[:, i:i + 1] * part_in[i, tile, :]
        attn = (((sums[0] + sums[1]) + (sums[2] + sums[3])) / denom).astype(BF16).astype(F32)
        for r in range(7):
            olhs_buf[:, r * LANES:(r + 1) * LANES] = jnp.broadcast_to(attn[r:r + 1, :], (16, LANES)).astype(BF16)
        if half == 0:
            for n in range(o_chunks):
                wo_copy(n).wait()
        for n in range(o_chunks):
            acc = jnp.dot(olhs_buf[...], wo_buf[n, half * half_width:(half + 1) * half_width, :], preferred_element_type=F32)
            for t in range(4):
                r = 4 * n + t
                here = jnp.where(rows8 == r % 8, acc[0:8, t * LANES:(t + 1) * LANES], 0.0)
                proj[r // 8] = proj[r // 8] + here
    for r in range(pad_md // 8):
        pair_out[r * 8:(r + 1) * 8, :] = proj[r]
    pair = pltpu.make_async_remote_copy(
        src_ref=pair_out, dst_ref=pair_in, send_sem=pair_send, recv_sem=pair_recv,
        device_id={"model": other}, device_id_type=MESH)
    pair.start()
    pair.wait()
    smalls[2].wait()
    resid = (hid + (pair_out[...] + pair_in[...])).astype(BF16).astype(F32)
    h2_all[my_slot] = norm(resid, gm_ref)

    for offset in box_far_first:
        if any(offset):
            pltpu.make_async_remote_copy(
                src_ref=h2_all.at[my_slot], dst_ref=h2_all.at[my_slot], send_sem=h2_send, recv_sem=h2_recv,
                device_id={"model": other, "seq": member_at(offset)[1]}, device_id_type=MESH).start()
    gone = h2_all.at[pl.ds(0, members - 1)]
    pltpu.make_async_copy(gone, gone, h2_recv).wait()
    rows = [h2_all[i].astype(F32) for i in range(members)]
    for n in range(n_md):
        tile = jnp.zeros((16, LANES), F32)
        for i in range(members):
            tile = jnp.where(rows16 == i, jnp.broadcast_to(rows[i][n:n + 1, :], (16, LANES)), tile)
        lhs_buf[:, n * LANES:(n + 1) * LANES] = tile.astype(BF16)

    up_wait(0)
    up_wait(1)
    wd_copy.wait()
    gate = jnp.dot(lhs_buf[...], wg_buf[...], preferred_element_type=F32).astype(BF16).astype(F32)
    up = jnp.dot(lhs_buf[...], wu_buf[...], preferred_element_type=F32).astype(BF16).astype(F32)
    act = jax.nn.silu(gate) * up
    cols = lax.broadcasted_iota(jnp.int32, act.shape, 1)
    act = jnp.where(cols < my_tiles * LANES, act, 0.0).astype(BF16)
    pieces = [(0, 8), (8, 16), (16, n_md)] if n_md > 16 else [(0, n_md)]
    homes = [member_at(offset) for offset in box_far_first]

    def down(n):
        return jnp.dot(act, wd_buf[:, n * 512:(n + 1) * 512], preferred_element_type=F32)

    ahead = down(0)
    for piece, (low, high) in enumerate(pieces):
        for n in range(low // 4, high // 4):
            acc = ahead
            if n + 1 < o_chunks:
                ahead = down(n + 1)
            for t in range(4):
                for i in range(members):
                    mlp_out[i, 4 * n + t:4 * n + t + 1, :] = acc[i:i + 1, t * LANES:(t + 1) * LANES]
        for slot, home in homes:
            tile = pl.ds(low, high - low)
            pltpu.make_async_remote_copy(
                src_ref=mlp_out.at[slot, tile], dst_ref=mlp_in.at[my_slot, tile], send_sem=red_send, recv_sem=red_recv.at[piece],
                device_id={"model": other, "seq": home}, device_id_type=MESH).start()

    finals = []
    for piece, (low, high) in enumerate(pieces):
        tile = pl.ds(low, high - low)
        landed = mlp_in.at[:, tile]
        pltpu.make_async_copy(landed, landed, red_recv.at[piece]).wait()
        total = mlp_in[0, low:high, :]
        for i in range(1, members):
            total = total + mlp_in[i, low:high, :]
        fin_out[low:high, :] = total
        fin = pltpu.make_async_remote_copy(
            src_ref=fin_out.at[tile], dst_ref=fin_in.at[tile], send_sem=fin_send.at[piece], recv_sem=fin_recv.at[piece],
            device_id={"model": other}, device_id_type=MESH)
        fin.start()
        finals.append(fin)
    for fin in finals:
        fin.wait()
    result = resid[0:n_md, :] + (fin_out[...] + fin_in[...])
    for n in range(n_md):
        out_ref[:, n * LANES:(n + 1) * LANES] = result[n:n + 1, :].astype(BF16)

    pltpu.make_async_copy(q_all, q_all, q_send).wait()
    pltpu.make_async_copy(part_in, part_in, part_send).wait()
    pltpu.make_async_copy(gone, gone, h2_send).wait()
    pltpu.make_async_copy(mlp_in, mlp_in, red_send).wait()


def solution(mesh):
    model_devs = mesh.shape["model"]
    seq_devs = mesh.shape["seq"]

    def device_step(hidden, k_cache, v_cache, sel_blocks, g_attn, g_mlp, w_q, w_o, w_gate, w_up, w_down):
        model_dim = hidden.shape[1]
        batch, tokens, kv_local, head_dim = k_cache.shape
        n_md = model_dim // LANES
        pad_md = -(-n_md // 16) * 16
        dims = torus_dims(seq_devs)
        box = mlp_box(dims)
        members = box[0] * box[1] * box[2]
        tiles_ffn = w_gate.shape[1] // LANES
        tiles_max = -(-tiles_ffn // members)
        width = w_q.shape[1] // model_devs
        kv_rows = tokens * kv_local
        k_rows = k_cache.reshape(batch, kv_rows, head_dim)
        v_rows = v_cache.reshape(batch, kv_rows, head_dim)
        cfg = (seq_devs, n_md, tiles_ffn, tiles_max)
        any_spec = pl.BlockSpec(memory_space=pl.ANY)
        vmem_spec = pl.BlockSpec(memory_space=pltpu.VMEM)
        dma = pltpu.SemaphoreType.DMA
        out = pl.pallas_call(
            functools.partial(decode_kernel, cfg),
            out_shape=pltpu.VMEM((1, model_dim), BF16),
            in_specs=[any_spec] * 11,
            out_specs=vmem_spec,
            scratch_shapes=[
                pltpu.VMEM((batch, kv_rows, LANES), BF16),
                pltpu.VMEM((batch, kv_rows, LANES), BF16),
                pltpu.VMEM((model_dim, width), BF16),
                pltpu.VMEM((model_dim // 512, width, 512), BF16),
                pltpu.VMEM((model_dim, tiles_max * LANES), BF16),
                pltpu.VMEM((model_dim, tiles_max * LANES), BF16),
                pltpu.VMEM((tiles_max * LANES, model_dim), BF16),
                pltpu.VMEM((1, model_dim), BF16),
                pltpu.VMEM((n_md, LANES), BF16),
                pltpu.VMEM((n_md, LANES), BF16),
                pltpu.VMEM((4, sel_blocks.shape[2], batch), jnp.int32),
                pltpu.VMEM((2, 2, batch, LANES), F32),
                pltpu.VMEM((16, model_dim), BF16),
                pltpu.VMEM((16, width // 2), BF16),
                pltpu.VMEM((16, LANES), BF16),
                pltpu.VMEM((batch, 16, LANES), BF16),
                pltpu.VMEM((batch * 16, kv_rows), F32),
                pltpu.VMEM((batch * 16, kv_rows), BF16),
                pltpu.VMEM((batch, 16, LANES), F32),
                pltpu.VMEM((batch, 16, LANES), F32),
                pltpu.VMEM((LANES, LANES), F32),
                pltpu.VMEM((pad_md, LANES), F32),
                pltpu.VMEM((pad_md, LANES), F32),
                pltpu.VMEM((members, pad_md, LANES), BF16),
                pltpu.VMEM((members, n_md, LANES), F32),
                pltpu.VMEM((members, n_md, LANES), F32),
                pltpu.VMEM((n_md, LANES), F32),
                pltpu.VMEM((n_md, LANES), F32),
                dma((4,)), dma((-(-width // 512),)), dma((2, 5)), dma((model_dim // 512,)), dma((3,)),
                dma, dma((5,)), dma, dma((2,)), dma, dma, dma, dma, dma, dma((3,)), dma((3,)), dma((3,)),
            ],
            compiler_params=pltpu.CompilerParams(
                collective_id=0, has_side_effects=True, vmem_limit_bytes=54 * 1024 * 1024),
            name="decode_step",
        )(hidden, g_attn.reshape(n_md, LANES), g_mlp.reshape(n_md, LANES), sel_blocks.transpose(1, 2, 0), k_rows, v_rows, w_q, w_o, w_gate, w_up, w_down)
        return out

    cache_spec = P("data", "seq", "model", None)
    in_specs = (P(("data", "seq"), None), cache_spec, cache_spec, P("data", None, None), P(None), P(None), P(None, None), P(None, None), P(None, "model"), P(None, "model"), P("model", None))
    return jax.shard_map(device_step, mesh=mesh, in_specs=in_specs, out_specs=P(("data", "seq"), None), check_vma=False)
```
